32 devices in a mesh: dp: 2 (over y), mp: 16 (over z, x, core).
Axes of the slice: x: 2, y: 2, z: 4, core: 2. Of those that a mesh axis runs over, the one named last changes fastest.
Arguments:
- features: bfloat16 [32, 1280, 1024], P('dp', 'mp'), may hold values from -6 to 6
- conv_weight: bfloat16 [1280, 1280], P('mp'), may hold values from -0.15625 to 0.15625
- norm_gain: float32 [1280], replicated, may hold values from 0.25 to 1.75
- norm_bias: float32 [1280], replicated, may hold values from -3 to 3
- logit_vector: float32 [1280], replicated, may hold values from -0.625 to 0.625
- labels: int32 [32], P(('dp', 'mp')), may hold values 0 or 1
Outputs:
- grad_features: float32 [32, 1280, 1024], P('dp', 'mp')
- grad_weight: float32 [1280, 1280], P('mp')
- head_grads: float32 [3, 1280], replicated
- loss: float32 [], replicated
The draws below stay inside these ranges and needn't reach their ends.
All inputs are finite; a program needn't handle non-finite values. No bound on the sum of `labels` on one device may be relied on, other than what follows from the above.
Results may differ from the reference program's by a relative error of at most 0.0029.
Values may be sent and summed in bfloat16 or wider, within the bound.
No kernel may reach another device: no remote copies, remote signals or barrier semaphores. Data moves between devices by JAX's collectives and lax.ppermute only.
A program may use at most 128 MiB of HBM per device.

```python
import jax
import jax.numpy as jnp
from jax import lax

C = 1280
CELLS = 1024
GROUPS = 32
IMAGES = 32


def plant(values, own_key, low, largest):
    dims = values.shape
    spot = [jax.random.randint(jax.random.fold_in(own_key, axis), (), 0, dims[axis]) for axis in range(len(dims))]
    values = values.at[tuple(spot)].set(low)
    longest = dims.index(max(dims))
    spot[longest] = (spot[longest] + 1) % dims[longest]
    return values.at[tuple(spot)].set(largest)


def levels(own_key, shape, split, smallest, top_value):
    level = 1.0
    for axis_at, shards_of in split:
        steps = jax.random.uniform(jax.random.fold_in(jax.random.fold_in(own_key, 6), axis_at), (shards_of,), jnp.float32, smallest / len(split), top_value / len(split))
        level = level * jnp.repeat(jnp.exp(steps), shape[axis_at] // shards_of).reshape((-1,) + (1,) * (len(shape) - 1 - axis_at))
    return level


def bell_draw(own_key, dims, scale, reach, cuts=(), dtype=jnp.bfloat16):
    result = jax.random.normal(own_key, dims, jnp.float32) * scale
    if len(cuts) > 0:
        result = levels(own_key, dims, cuts, -0.22, 0.18) * result
    return jnp.clip(result, min=-reach, max=reach).astype(dtype)


def setup_inputs(seed: int = 0) -> dict:
    seeds = jax.random.split(jax.random.key(seed), 7)
    return {
        "features": bell_draw(seeds[0], (IMAGES, C, CELLS), 1.0, 6.0, ((0, 2), (1, 16))),
        "conv_weight": bell_draw(seeds[1], (C, C), C ** -0.5, 0.15625, ((0, 16),)),
        "norm_gain": jnp.clip(1.0 + 0.15 * jax.random.normal(seeds[2], (C,), jnp.float32), 0.25, 1.75),
        "norm_bias": bell_draw(seeds[3], (C,), 0.5, 3.0, (), jnp.float32),
        "logit_vector": bell_draw(seeds[4], (C,), (C // 16) ** -0.5, 0.625, (), jnp.float32),
        "labels": plant((jax.random.randint(seeds[5], (IMAGES,), 0, 2) < 1).astype(jnp.int32), jax.random.fold_in(seeds[5], 1), 0, 1),
    }


norm_eps = 1e-05

def head_total(pre, norm_gain, norm_bias, logit_vector, signs):
    images = pre.shape[0]
    grouped = pre.reshape(images, GROUPS, C // GROUPS, CELLS)
    center = lax.optimization_barrier(jnp.mean(grouped, axis=(2, 3), keepdims=True))
    spread = lax.optimization_barrier(jnp.mean((grouped - center) ** 2, axis=(2, 3), keepdims=True))
    normed = ((grouped - center) * lax.rsqrt(spread + norm_eps)).reshape(images, C, CELLS)
    normed = normed * norm_gain[:, None] + norm_bias[:, None]
    hidden = jax.nn.silu(normed)
    logits = jnp.einsum('c,ncs->n', logit_vector, hidden, precision=lax.Precision.HIGHEST) / CELLS
    margin = jnp.maximum(1.0 - signs * logits, 0.0)
    return jnp.sum(margin * margin)

def reference(features, conv_weight, norm_gain, norm_bias, logit_vector, labels):
    weight_wide = conv_weight.astype(jnp.float32)
    signs = 2.0 * labels.astype(jnp.float32) - 1.0

    def one_image(carry, inputs):
        grad_acc, small_acc, total_acc = carry
        image, sign = inputs
        image_wide = image.astype(jnp.float32)
        pre = jnp.einsum('io,is->os', weight_wide, image_wide, precision=lax.Precision.HIGHEST)[None]
        total, pull = jax.vjp(lambda p, g, b, h: head_total(p, g, b, h, sign[None]), pre, norm_gain, norm_bias, logit_vector)
        grad_pre, grad_gain, grad_bias, grad_vec = pull(jnp.ones((), jnp.float32))
        grad_pre = grad_pre[0].astype(jnp.bfloat16).astype(jnp.float32)
        grad_acc = grad_acc + jnp.einsum('is,os->io', image_wide, grad_pre, precision=lax.Precision.HIGHEST)
        grad_image = jnp.einsum('io,os->is', weight_wide, grad_pre, precision=lax.Precision.HIGHEST)
        small_acc = small_acc + jnp.stack([grad_gain, grad_bias, grad_vec])
        return ((grad_acc, small_acc, total_acc + total), grad_image)
    start = (jnp.zeros((C, C), jnp.float32), jnp.zeros((3, C), jnp.float32), jnp.zeros((), jnp.float32))
    (grad_weight, head_grads, total), grad_features = lax.scan(one_image, start, (features, signs))
    loss = total / features.shape[0]
    return (grad_features, grad_weight, head_grads, loss)
```

```python
import functools

import jax
import jax.numpy as jnp
from jax import lax
from jax.experimental import pallas as pl
from jax.experimental.pallas import tpu as pltpu
from jax.sharding import PartitionSpec as P

GROUPS = 32
norm_eps = 1e-05
F32 = jnp.float32
BF16 = jnp.bfloat16
VMEM = pl.BlockSpec(memory_space=pltpu.VMEM)
SMEM = pl.BlockSpec(memory_space=pltpu.SMEM)
EXTRA = 8


def stacked(refs):
    return jnp.concatenate([ref[...] for ref in refs])


def weight_columns(rows, grad_pre, out):
    ch = grad_pre.shape[0]
    step = ch // 5
    for j in range(5):
        cols = pl.ds(j * step, step)
        out[: rows.shape[0], cols] = lax.dot_general(
            rows, grad_pre[cols, :], (((1,), (1,)), ((), ())), preferred_element_type=F32
        )


def head_kernel(
    info_ref, begun_ref, turned_ref, par_ref, *refs,
):
    last_refs, refs = refs[:4], refs[4:]
    pre_grad_ref, small_ref, pre_ref, slope_ref, sums_ref, center_ref, rstd_ref = refs
    ch, cells = pre_ref.shape
    width = ch // GROUPS
    count = width * cells
    add_product(begun_ref, turned_ref, last_refs, pre_ref)

    def at(g):
        return pl.ds(pl.multiple_of(g * width, 8), width)

    def tile(g, r):
        return pl.ds(pl.multiple_of(g * width + 8 * r, 8), 8)

    tiles, lanes = range(width // 8), [pl.ds(128 * c, 128) for c in range(cells // 128)]

    def sweep(body, trips, unroll):
        lax.fori_loop(0, trips, lambda g, _: body(g) or 0, 0, unroll=unroll)

    def spot(value):
        return jnp.broadcast_to(value, (8, 128))

    def means(g):
        center_ref[g] = spot(jnp.sum(pre_ref[at(g), :], axis=(0, 1), keepdims=True) / count)

    def spreads(g):
        center, acc = center_ref[g], jnp.zeros((8, 128), F32)
        for r in tiles:
            for c in lanes:
                dev = pre_ref[tile(g, r), c] - center
                acc += dev * dev
        spread = jnp.sum(acc, axis=(0, 1), keepdims=True) / count
        rstd_ref[g] = spot(lax.rsqrt(spread + norm_eps))

    def activate(g):
        center, rstd = center_ref[g], rstd_ref[g]
        for r in tiles:
            rows = tile(g, r)
            a, b = par_ref[0, rows, :] * (0.5 * rstd), 0.5 * par_ref[1, rows, :]
            sum_h = sum_d = sum_du = jnp.zeros((8, 128), F32)
            for c in lanes:
                dev = pre_ref[rows, c] - center
                w = dev * a + b
                t = jnp.tanh(w)
                q = 1.0 + t
                h = w * q
                d2 = q + h * (1.0 - t)
                slope_ref[rows, c] = d2
                sum_h += h
                sum_d += d2
                sum_du += d2 * dev
            sums_ref[0, rows, :] = sum_du * (0.5 * rstd)
            sums_ref[1, rows, :] = 0.5 * sum_d
            sums_ref[2, rows, :] = sum_h

    sweep(means, GROUPS, 8)
    sweep(spreads, GROUPS, 8)
    sweep(activate, GROUPS, 2)

    def total(g):
        for i in range(3):
            lane_sum = jnp.sum(sums_ref[i, at(g), :], axis=1, keepdims=True)
            sums_ref[i, at(g), :] = jnp.broadcast_to(lane_sum, (width, 128))

    sweep(total, GROUPS, 8)
    logit = jnp.sum(par_ref[2] * sums_ref[2], axis=0, keepdims=True) / cells
    sign = info_ref[0].astype(F32)
    margin = jnp.maximum(1.0 - sign * logit, 0.0)
    k = (-2.0 * sign / cells) * margin

    def finish(pair):
        out = {}
        for side in range(2):
            g = 2 * pair + side
            center, rstd = center_ref[g], rstd_ref[g]
            gv = par_ref[0, at(g), :] * par_ref[2, at(g), :]
            scale = (k / count) * rstd
            m1 = scale * jnp.sum(gv * sums_ref[1, at(g), :], axis=0, keepdims=True)
            m2 = scale * rstd * jnp.sum(gv * sums_ref[0, at(g), :], axis=0, keepdims=True)
            for r in tiles:
                rows = tile(g, r)
                slope = (0.5 * k) * rstd * (par_ref[0, rows, :] * par_ref[2, rows, :])
                for i, c in enumerate(lanes):
                    dev = pre_ref[rows, c] - center
                    out[side * len(tiles) + r, i] = slope_ref[rows, c] * slope - (m1 + dev * m2)
        for r in tiles:
            rows = pl.ds(pl.multiple_of(2 * pair * width + 16 * r, 16), 16)
            for i, c in enumerate(lanes):
                both = jnp.concatenate([out[2 * r, i], out[2 * r + 1, i]])
                pre_grad_ref[rows, c] = both.astype(BF16)

    sweep(finish, GROUPS // 2, 1)
    lane = lax.broadcasted_iota(jnp.int32, (ch, 128), 1)
    vec = par_ref[2]
    turned = jnp.where(lane == 0, vec * sums_ref[0], 0.0)
    turned = jnp.where(lane == 1, vec * sums_ref[1], turned)
    turned = jnp.where(lane == 2, sums_ref[2], turned).T[:EXTRA]
    line = lax.broadcasted_iota(jnp.int32, turned.shape, 0)
    k, margin = k[:, :1], margin[:, :1]
    small_ref[...] = jnp.where(line == 3, margin * margin, turned * k)


def head(sign, begun, turned, params, last):
    ch, cells = begun.shape
    return pl.pallas_call(
        head_kernel,
        out_shape=(jax.ShapeDtypeStruct((ch, cells), BF16), jax.ShapeDtypeStruct((EXTRA, ch), F32)),
        in_specs=[SMEM] + [VMEM] * 7,
        out_specs=(VMEM, VMEM),
        scratch_shapes=[pltpu.VMEM((ch, cells), F32)] * 2
        + [pltpu.VMEM((3, ch, 128), F32)]
        + [pltpu.VMEM((GROUPS, 8, 128), F32)] * 2,
        cost_estimate=pl.CostEstimate(
            flops=3 * ch * ch * cells, bytes_accessed=8 * ch * cells, transcendentals=ch * cells
        ),
        compiler_params=pltpu.CompilerParams(vmem_limit_bytes=28 << 20),
        name="head",
    )(sign, begun, turned, params, *last)


def add_product(begun_ref, turned_ref, refs, out_ref):
    image = stacked(refs)
    step = out_ref.shape[0] // 4
    for j in range(4):
        rows = pl.ds(j * step, step)
        product = jnp.dot(turned_ref[rows, :], image, preferred_element_type=F32)
        out_ref[rows, :] = product if begun_ref is None else begun_ref[rows, :] + product


def first_kernel(turned_ref, *refs):
    add_product(None, turned_ref, refs[:-1], refs[-1])


def next_kernel(begun_ref, turned_ref, *refs):
    add_product(begun_ref, turned_ref, refs[:-1], refs[-1])


def product(begun, turned, images):
    ch, depth = turned.shape
    cells = images[0].shape[1]
    args = ([] if begun is None else [begun]) + [turned, *images]
    return pl.pallas_call(
        first_kernel if begun is None else next_kernel,
        out_shape=jax.ShapeDtypeStruct((ch, cells), F32),
        in_specs=[VMEM] * len(args),
        out_specs=VMEM,
        input_output_aliases={} if begun is None else {0: 0},
        cost_estimate=pl.CostEstimate(
            flops=2 * ch * depth * cells, bytes_accessed=8 * ch * cells, transcendentals=0
        ),
        compiler_params=pltpu.CompilerParams(vmem_limit_bytes=14 << 20),
        name="product",
    )(*args)


def image_kernel(weight_ref, pre_grad_ref, *out_refs):
    sub = out_refs[0].shape[0]
    grads = jnp.dot(weight_ref[...], pre_grad_ref[...], preferred_element_type=F32)
    for i, out_ref in enumerate(out_refs):
        out_ref[...] = grads[i * sub : (i + 1) * sub].astype(BF16)


def grad_blocks(weight, grad_pre, parts):
    rows, ch = weight.shape
    cells = grad_pre.shape[1]
    return pl.pallas_call(
        image_kernel,
        out_shape=(jax.ShapeDtypeStruct((rows // parts, cells), BF16),) * parts,
        in_specs=[VMEM, VMEM],
        out_specs=(VMEM,) * parts,
        cost_estimate=pl.CostEstimate(
            flops=2 * rows * ch * cells, bytes_accessed=2 * ch * cells, transcendentals=0
        ),
        compiler_params=pltpu.CompilerParams(vmem_limit_bytes=12 << 20),
        name="grad_blocks",
    )(weight, grad_pre)


def keep_kernel(pre_grad_ref, *refs):
    weight_columns(stacked(refs[:-1]), pre_grad_ref, refs[-1])


def weight_keep(grad_pre, images):
    ch, cells = grad_pre.shape
    return pl.pallas_call(
        keep_kernel,
        out_shape=jax.ShapeDtypeStruct((ch // 2, ch), F32),
        in_specs=[VMEM] * (1 + len(images)),
        out_specs=VMEM,
        cost_estimate=pl.CostEstimate(
            flops=ch * ch * cells, bytes_accessed=4 * ch * cells, transcendentals=0
        ),
        compiler_params=pltpu.CompilerParams(vmem_limit_bytes=14 << 20),
        name="weight_keep",
    )(grad_pre, *images)


def arrange_kernel(at_ref, near_ref, across_ref, core_ref, *out_refs):
    _, sub, half = near_ref.shape

    def put(row):
        for k, masks in enumerate(SETS):
            for i, m in enumerate(masks):
                for side in range(2):
                    at = (((m >> 1) & 1) * 2 + ((m >> 2) & 1)) * 2 + (m >> 3)
                    if m & 1:
                        block = core_ref[(side ^ row) * 8 + at]
                    else:
                        block = near_ref[at] if side == row else across_ref[at]
                    out_refs[k][i * sub : (i + 1) * sub, side * half : (side + 1) * half] = block

    for row in range(2):
        pl.when(at_ref[1] == row)(functools.partial(put, row))


def bit_order(bit):
    return [4 * z + 2 * x + bit for z in range(4) for x in range(2)]


def local(kernel, outs, *args, spec=None, **extra):
    specs = [SMEM] + [VMEM] * (len(args) - 1) if spec is None else spec
    return pl.pallas_call(
        kernel,
        out_shape=outs,
        in_specs=specs,
        cost_estimate=pl.CostEstimate(flops=1 << 21, bytes_accessed=1 << 20, transcendentals=0),
        compiler_params=pltpu.CompilerParams(vmem_limit_bytes=14 << 20),
        **extra,
    )(*args)


def rows_at(start, count):
    return pl.ds(pl.multiple_of(start, 8), count)


def sum1_kernel(at_ref, own_ref, pre_grad_ref, small_a, small_b, *refs):
    images, (psend, pkeep, qsend, qkeep, total) = refs[:-5], refs[-5:]
    weight_columns(stacked(images), pre_grad_ref, total)
    body, cols = total.shape[0], total.shape[1] // 2
    sub = body // 8
    left, right = pl.ds(0, cols), pl.ds(cols, cols)
    half, row = sub // 2, at_ref[1]
    tail = small_a[...] + small_b[...]
    tail = jnp.concatenate([tail[:4, :cols], tail[:4, cols:]])
    for out, side, across in ((psend, 1 - row, 1), (pkeep, row, 0)):
        for b in range(8):
            rows = rows_at(b * sub + side * half, half)
            out[b * half : (b + 1) * half, :] = own_ref[rows, left] + total[rows, left]
        out[body // 2 :, :] = tail
        out = qsend if out is psend else qkeep
        for z in range(4):
            rows = pl.ds((2 * z + across) * sub, sub)
            out[z * sub : (z + 1) * sub, :] = own_ref[rows, right] + total[rows, right]


def sum2_kernel(at_ref, pa, pb, qa, qb, psend, pkeep, qsend, qkeep):
    body = pa.shape[0] - EXTRA
    half = body // 8
    row = at_ref[1]
    for pout, qout, side, across in ((psend, qsend, 1 - row, 1), (pkeep, qkeep, row, 0)):
        for z in range(4):
            to = pl.ds(z * half, half)
            rows = pl.ds((2 * z + across) * half, half)
            pout[to, :] = pa[rows, :] + pb[rows, :]
            rows = rows_at((2 * z + side) * half, half)
            qout[to, :] = qa[rows, :] + qb[rows, :]
        pout[body // 2 :, :] = pa[body:, :] + pb[body:, :]


def sum3_kernel(at_ref, pa, pb, qa, qb, send, keep):
    body, cols = qa.shape
    half = body // 4
    for out, side in ((send, 1), (keep, 0)):
        for z in range(2):
            to = pl.ds(z * half, half)
            rows = pl.ds((2 * z + side) * half, half)
            out[to, :cols] = pa[rows, :] + pb[rows, :]
            out[to, cols:] = qa[rows, :] + qb[rows, :]
        out[body // 2 :, :cols] = pa[body:, :] + pb[body:, :]
        out[body // 2 :, cols:] = jnp.zeros((EXTRA, cols), F32)


def sum4_kernel(at_ref, a_ref, b_ref, send, keep):
    body = a_ref.shape[0] - EXTRA
    for out, side in ((send, 1), (keep, 0)):
        rows = pl.ds(side * (body // 2), body // 2)
        out[: body // 2, :] = a_ref[rows, :] + b_ref[rows, :]
        out[body // 2 :, :] = a_ref[body:, :] + b_ref[body:, :]


def sum5_kernel(images, at_ref, a_ref, b_ref, part, sums, loss):
    body, cols = part.shape[0], part.shape[1] // 2
    part[...] = (a_ref[:body, :] + b_ref[:body, :]).astype(part.dtype)
    tail = a_ref[body:, :cols] + b_ref[body:, :cols]
    sums[...] = jnp.concatenate([tail[:3], tail[4:7]], axis=1)
    loss[0] = jnp.sum(tail[3:4, :1]) / images


def join_kernel(at_ref, part, other, out):
    half = part.shape[0]
    out[rows_at(at_ref[1] * half, half), :] = part[...].astype(F32)
    out[rows_at((1 - at_ref[1]) * half, half), :] = other[...].astype(F32)


def scatter_steps(at, sources, n, sub, ch):
    f32 = lambda rows, cols: jax.ShapeDtypeStruct((rows, cols), F32)
    cols, half = ch // 2, sub // 2
    on_x = lambda v: exchange(v, "mp", n, 2)
    on_y = lambda v: exchange(v, "dp", 2, 1)
    outs = (f32(8 * half + EXTRA, cols),) * 2 + (f32(4 * sub, cols),) * 2
    psend, pkeep, qsend, qkeep = local(
        sum1_kernel, outs, at, *sources, scratch_shapes=[pltpu.VMEM((8 * sub, ch), F32)]
    )
    parts = pkeep, on_y(psend), qkeep, on_x(qsend)
    outs = (f32(4 * half + EXTRA, cols),) * 2 + (f32(4 * half, cols),) * 2
    psend, pkeep, qsend, qkeep = local(sum2_kernel, outs, at, *parts)
    parts = pkeep, on_x(psend), qkeep, on_y(qsend)
    send, keep = local(sum3_kernel, (f32(2 * half + EXTRA, ch),) * 2, at, *parts)
    arrived = exchange(send, "mp", n, 4)
    send, keep = local(sum4_kernel, (f32(half + EXTRA, ch),) * 2, at, keep, arrived)
    arrived = exchange(send, "mp", n, 8)
    final = jax.ShapeDtypeStruct((half, ch), BF16)
    part, sums, loss = local(
        functools.partial(sum5_kernel, 2 * n),
        (final, f32(3, ch), jax.ShapeDtypeStruct((1,), F32)),
        at,
        keep,
        arrived,
        out_specs=(VMEM, VMEM, SMEM),
    )
    other = on_y(part)
    return local(join_kernel, f32(sub, ch), at, part, other), sums, loss[0]


def land_kernel(masks, at_ref, *refs):
    count = len(masks)
    blocks, out_ref, (wide, sems) = refs[:count], refs[-3], refs[-2:]
    copies = []
    for i, m in enumerate(masks):
        wide[i] = blocks[i][...].astype(F32)
        copies.append(pltpu.make_async_copy(wide.at[i], out_ref.at[at_ref[0] ^ m], sems.at[i]))
        copies[-1].start()
    for copy in copies:
        copy.wait()


def land(at, blocks, masks, out, n):
    sub, cells = blocks[masks[0]].shape
    anywhere = pl.BlockSpec(memory_space=pl.ANY)
    args = [at] + [blocks[m] for m in masks]
    spec = [SMEM] + [VMEM] * len(masks)
    extra = {}
    if out is not None:
        args, spec = args + [out], spec + [anywhere]
        extra["input_output_aliases"] = {len(args) - 1: 0}
    return local(
        functools.partial(land_kernel, masks),
        jax.ShapeDtypeStruct((n, sub, cells), F32),
        *args,
        spec=spec,
        out_specs=anywhere,
        scratch_shapes=[
            pltpu.VMEM((len(masks), sub, cells), F32),
            pltpu.SemaphoreType.DMA((len(masks),)),
        ],
        **extra,
    )


def exchange(value, axis, size, mask):
    return lax.ppermute(value, axis, [(i, i ^ mask) for i in range(size)])


def gather_weight(block, at, n, row):
    sub, ch = block.shape
    half = ch // 2
    rows = lax.dynamic_slice_in_dim(block, row * half, half, 1)[None]
    for mask in (8, 4):
        rows = jnp.concatenate([rows, exchange(rows, "mp", n, mask)])
    near = jnp.concatenate([rows, exchange(rows, "mp", n, 2)])
    across = exchange(near, "dp", 2, 1)
    core = exchange(jnp.concatenate([near, across]), "mp", n, 1)
    outs = tuple(jax.ShapeDtypeStruct((len(m) * sub, ch), BF16) for m in SETS)
    return local(arrange_kernel, outs, at, near, across, core)


def fast_shards(features, conv_weight, norm_gain, norm_bias, logit_vector, labels):
    n, sub, _ = features.shape
    ch = conv_weight.shape[1]
    place, row = lax.axis_index("mp"), lax.axis_index("dp")
    at = jnp.stack([place, row])
    params = jnp.stack([norm_gain, norm_bias, logit_vector])
    params = jnp.broadcast_to(params[:, :, None], (3, ch, 128))
    image = {}
    for m in range(n):
        block = lax.dynamic_index_in_dim(features, place ^ m, 0, keepdims=False)
        image[m] = exchange(block, "mp", n, m) if m else block
    weights = gather_weight(conv_weight, at, n, row)
    pre = None
    for k in PRODUCTS[:-1]:
        pre = product(pre, weights[k].T, [image[m] for m in SETS[k]])
        pre, params = lax.optimization_barrier((pre, params))
    twin = [exchange(image[m], "mp", n, 1) for m in bit_order(1)]
    k = PRODUCTS[-1]
    last = [image[m] for m in SETS[k]]
    grad_pre, small = head(2 * labels - 1, pre, weights[k].T, params, last)
    twin_pre = exchange(grad_pre, "mp", n, 1)
    twin_small = exchange(small, "mp", n, 1)
    blocks = {}
    for k, masks in enumerate(SETS):
        blocks.update(zip(masks, grad_blocks(weights[k], grad_pre, len(masks))))
    landed = {}
    for m, block in blocks.items():
        if m in RELAYED:
            block = exchange(block, "mp", n, m ^ 2)
            landed[m] = exchange(block, "mp", n, 2)
        else:
            landed[m] = exchange(block, "mp", n, m) if m else block
    keep = weight_keep(grad_pre, [image[m] for m in bit_order(0)])
    sources = (keep, twin_pre, small, twin_small, *twin)
    grad_weight, head_grads, loss = scatter_steps(at, sources, n, sub, ch)
    grad_features = None
    for masks in LAND:
        grad_features = land(at, landed, masks, grad_features, n)
    return grad_features, grad_weight, head_grads, loss


def head_total(pre, norm_gain, norm_bias, logit_vector, signs):
    images, channels, cell_count = pre.shape
    grouped = pre.reshape(images, GROUPS, channels // GROUPS, cell_count)
    center = jnp.mean(grouped, axis=(2, 3), keepdims=True)
    spread = jnp.mean((grouped - center) ** 2, axis=(2, 3), keepdims=True)
    normed = ((grouped - center) * lax.rsqrt(spread + norm_eps)).reshape(
        images, channels, cell_count
    )
    normed = normed * norm_gain[:, None] + norm_bias[:, None]
    hidden = jax.nn.silu(normed)
    logits = (
        jnp.einsum("c,ncs->n", logit_vector, hidden, precision=lax.Precision.HIGHEST) / cell_count
    )
    margin = jnp.maximum(1.0 - signs * logits, 0.0)
    return jnp.sum(margin * margin)


def shards(features, conv_weight, norm_gain, norm_bias, logit_vector, labels):
    signs = 2.0 * labels.astype(jnp.float32) - 1.0
    weight_full = lax.all_gather(conv_weight, "mp", axis=0, tiled=True)
    image_block = lax.all_to_all(features, "mp", split_axis=0, concat_axis=1, tiled=True)
    pre = jnp.einsum("io,nis->nos", weight_full, image_block, preferred_element_type=jnp.float32)
    total, pull = jax.vjp(
        lambda p, g, b, h: head_total(p, g, b, h, signs), pre, norm_gain, norm_bias, logit_vector
    )
    grad_pre, grad_gain, grad_bias, grad_vec = pull(jnp.ones((), jnp.float32))
    grad_pre = grad_pre.astype(jnp.bfloat16)
    grad_image = jnp.einsum(
        "io,nos->nis", weight_full, grad_pre, preferred_element_type=jnp.float32
    )
    grad_features = lax.all_to_all(grad_image, "mp", split_axis=1, concat_axis=0, tiled=True)
    weight_term = jnp.einsum(
        "nis,nos->io", image_block, grad_pre, preferred_element_type=jnp.float32
    )
    summed = lax.psum(weight_term, "dp")
    grad_weight = lax.psum_scatter(summed, "mp", scatter_dimension=0, tiled=True)
    total_sum, head_grads = lax.psum(
        (total, jnp.stack([grad_gain, grad_bias, grad_vec])), ("dp", "mp")
    )
    image_total = pre.shape[0] * lax.axis_size("dp") * lax.axis_size("mp")
    loss = total_sum / image_total
    return (grad_features, grad_weight, head_grads, loss)


SETS = ((12, 8, 13, 9), (4, 5, 1, 0), (15, 11, 6, 7), (14, 10, 2, 3))
PRODUCTS = (0, 1, 3, 2)
LAND = ((0, 12, 8, 13, 9), (4, 5, 1, 14, 10), (15, 11, 6, 7, 2, 3))
RELAYED = (14, 10)


def solution(mesh):
    fast = mesh.shape["mp"] == 16 and mesh.shape["dp"] == 2
    return jax.shard_map(
        fast_shards if fast else shards,
        mesh=mesh,
        in_specs=(P("dp", "mp", None), P("mp", None), P(), P(), P(), P(("dp", "mp"))),
        out_specs=(P("dp", "mp", None), P("mp", None), P(), P()),
        check_vma=False,
    )
```

```python
import functools

import jax
import jax.numpy as jnp
from jax import lax
from jax.experimental import pallas as pl
from jax.experimental.pallas import tpu as pltpu
from jax.sharding import PartitionSpec as P

GROUPS = 32
norm_eps = 1e-05
F32 = jnp.float32
BF16 = jnp.bfloat16
VMEM = pl.BlockSpec(memory_space=pltpu.VMEM)
SMEM = pl.BlockSpec(memory_space=pltpu.SMEM)
EXTRA = 8


def stacked(refs):
    return jnp.concatenate([ref[...] for ref in refs])


def weight_columns(rows, grad_pre, out):
    ch = grad_pre.shape[0]
    step = ch // 5
    for j in range(5):
        cols = pl.ds(j * step, step)
        out[: rows.shape[0], cols] = lax.dot_general(
            rows, grad_pre[cols, :], (((1,), (1,)), ((), ())), preferred_element_type=F32
        )


def head_kernel(
    info_ref, begun_ref, par_ref, turned_ref, turned_too_ref, *refs,
):
    last_refs, last_too_refs, refs = refs[:4], refs[4:8], refs[8:]
    pre_grad_ref, small_ref, pre_ref, slope_ref, sums_ref, center_ref, rstd_ref = refs
    ch, cells = pre_ref.shape
    width = ch // GROUPS
    count = width * cells
    add_product(begun_ref, turned_ref, last_refs, pre_ref)
    add_product(pre_ref, turned_too_ref, last_too_refs, pre_ref)

    def at(g):
        return pl.ds(pl.multiple_of(g * width, 8), width)

    def tile(g, r):
        return pl.ds(pl.multiple_of(g * width + 8 * r, 8), 8)

    tiles, lanes = range(width // 8), [pl.ds(128 * c, 128) for c in range(cells // 128)]

    def sweep(body, trips, unroll):
        lax.fori_loop(0, trips, lambda g, _: body(g) or 0, 0, unroll=unroll)

    def spot(value):
        return jnp.broadcast_to(value, (8, 128))

    def means(g):
        center_ref[g] = spot(jnp.sum(pre_ref[at(g), :], axis=(0, 1), keepdims=True) / count)

    def spreads(g):
        center, acc = center_ref[g], jnp.zeros((8, 128), F32)
        for r in tiles:
            for c in lanes:
                dev = pre_ref[tile(g, r), c] - center
                acc += dev * dev
        spread = jnp.sum(acc, axis=(0, 1), keepdims=True) / count
        rstd_ref[g] = spot(lax.rsqrt(spread + norm_eps))

    def activate(g):
        center, rstd = center_ref[g], rstd_ref[g]
        for r in tiles:
            rows = tile(g, r)
            a, b = par_ref[0, rows, :] * (0.5 * rstd), 0.5 * par_ref[1, rows, :]
            sum_h = sum_d = sum_du = jnp.zeros((8, 128), F32)
            for c in lanes:
                dev = pre_ref[rows, c] - center
                w = dev * a + b
                t = jnp.tanh(w)
                q = 1.0 + t
                h = w * q
                d2 = q + h * (1.0 - t)
                slope_ref[rows, c] = d2
                sum_h += h
                sum_d += d2
                sum_du += d2 * dev
            sums_ref[0, rows, :] = sum_du * (0.5 * rstd)
            sums_ref[1, rows, :] = 0.5 * sum_d
            sums_ref[2, rows, :] = sum_h

    sweep(means, GROUPS, 8)
    sweep(spreads, GROUPS, 8)
    sweep(activate, GROUPS, 2)

    def total(g):
        for i in range(3):
            lane_sum = jnp.sum(sums_ref[i, at(g), :], axis=1, keepdims=True)
            sums_ref[i, at(g), :] = jnp.broadcast_to(lane_sum, (width, 128))

    sweep(total, GROUPS, 8)
    logit = jnp.sum(par_ref[2] * sums_ref[2], axis=0, keepdims=True) / cells
    sign = info_ref[0].astype(F32)
    margin = jnp.maximum(1.0 - sign * logit, 0.0)
    k = (-2.0 * sign / cells) * margin

    def finish(pair):
        out = {}
        for side in range(2):
            g = 2 * pair + side
            center, rstd = center_ref[g], rstd_ref[g]
            gv = par_ref[0, at(g), :] * par_ref[2, at(g), :]
            scale = (k / count) * rstd
            m1 = scale * jnp.sum(gv * sums_ref[1, at(g), :], axis=0, keepdims=True)
            m2 = scale * rstd * jnp.sum(gv * sums_ref[0, at(g), :], axis=0, keepdims=True)
            for r in tiles:
                rows = tile(g, r)
                slope = (0.5 * k) * rstd * (par_ref[0, rows, :] * par_ref[2, rows, :])
                for i, c in enumerate(lanes):
                    dev = pre_ref[rows, c] - center
                    out[side * len(tiles) + r, i] = slope_ref[rows, c] * slope - (m1 + dev * m2)
        for r in tiles:
            rows = pl.ds(pl.multiple_of(2 * pair * width + 16 * r, 16), 16)
            for i, c in enumerate(lanes):
                both = jnp.concatenate([out[2 * r, i], out[2 * r + 1, i]])
                pre_grad_ref[rows, c] = both.astype(BF16)

    sweep(finish, GROUPS // 2, 1)
    lane = lax.broadcasted_iota(jnp.int32, (ch, 128), 1)
    vec = par_ref[2]
    turned = jnp.where(lane == 0, vec * sums_ref[0], 0.0)
    turned = jnp.where(lane == 1, vec * sums_ref[1], turned)
    turned = jnp.where(lane == 2, sums_ref[2], turned).T[:EXTRA]
    line = lax.broadcasted_iota(jnp.int32, turned.shape, 0)
    k, margin = k[:, :1], margin[:, :1]
    small_ref[...] = jnp.where(line == 3, margin * margin, turned * k)


def head(sign, begun, params, turned, last):
    ch, cells = begun.shape
    return pl.pallas_call(
        head_kernel,
        out_shape=(jax.ShapeDtypeStruct((ch, cells), BF16), jax.ShapeDtypeStruct((EXTRA, ch), F32)),
        in_specs=[SMEM] + [VMEM] * 12,
        out_specs=(VMEM, VMEM),
        scratch_shapes=[pltpu.VMEM((ch, cells), F32)] * 2
        + [pltpu.VMEM((3, ch, 128), F32)]
        + [pltpu.VMEM((GROUPS, 8, 128), F32)] * 2,
        cost_estimate=pl.CostEstimate(
            flops=3 * ch * ch * cells, bytes_accessed=8 * ch * cells, transcendentals=ch * cells
        ),
        compiler_params=pltpu.CompilerParams(vmem_limit_bytes=28 << 20),
        name="head",
    )(sign, begun, params, *turned, *last)


def add_product(begun_ref, turned_ref, refs, out_ref):
    image = stacked(refs)
    step = out_ref.shape[0] // 4
    for j in range(4):
        rows = pl.ds(j * step, step)
        product = jnp.dot(turned_ref[rows, :], image, preferred_element_type=F32)
        out_ref[rows, :] = product if begun_ref is None else begun_ref[rows, :] + product


def first_kernel(turned_ref, *refs):
    add_product(None, turned_ref, refs[:-1], refs[-1])


def next_kernel(begun_ref, turned_ref, *refs):
    add_product(begun_ref, turned_ref, refs[:-1], refs[-1])


def product(begun, turned, images):
    ch, depth = turned.shape
    cells = images[0].shape[1]
    args = ([] if begun is None else [begun]) + [turned, *images]
    return pl.pallas_call(
        first_kernel if begun is None else next_kernel,
        out_shape=jax.ShapeDtypeStruct((ch, cells), F32),
        in_specs=[VMEM] * len(args),
        out_specs=VMEM,
        input_output_aliases={} if begun is None else {0: 0},
        cost_estimate=pl.CostEstimate(
            flops=2 * ch * depth * cells, bytes_accessed=8 * ch * cells, transcendentals=0
        ),
        compiler_params=pltpu.CompilerParams(vmem_limit_bytes=14 << 20),
        name="product",
    )(*args)


def image_kernel(weight_ref, pre_grad_ref, *out_refs):
    sub = out_refs[0].shape[0]
    grads = jnp.dot(weight_ref[...], pre_grad_ref[...], preferred_element_type=F32)
    for i, out_ref in enumerate(out_refs):
        out_ref[...] = grads[i * sub : (i + 1) * sub].astype(BF16)


def grad_blocks(weight, grad_pre, parts):
    rows, ch = weight.shape
    cells = grad_pre.shape[1]
    return pl.pallas_call(
        image_kernel,
        out_shape=(jax.ShapeDtypeStruct((rows // parts, cells), BF16),) * parts,
        in_specs=[VMEM, VMEM],
        out_specs=(VMEM,) * parts,
        cost_estimate=pl.CostEstimate(
            flops=2 * rows * ch * cells, bytes_accessed=2 * ch * cells, transcendentals=0
        ),
        compiler_params=pltpu.CompilerParams(vmem_limit_bytes=12 << 20),
        name="grad_blocks",
    )(weight, grad_pre)


def keep_kernel(pre_grad_ref, *refs):
    weight_columns(stacked(refs[:-1]), pre_grad_ref, refs[-1])


def weight_keep(grad_pre, images):
    ch, cells = grad_pre.shape
    return pl.pallas_call(
        keep_kernel,
        out_shape=jax.ShapeDtypeStruct((ch // 2, ch), F32),
        in_specs=[VMEM] * (1 + len(images)),
        out_specs=VMEM,
        cost_estimate=pl.CostEstimate(
            flops=ch * ch * cells, bytes_accessed=4 * ch * cells, transcendentals=0
        ),
        compiler_params=pltpu.CompilerParams(vmem_limit_bytes=14 << 20),
        name="weight_keep",
    )(grad_pre, *images)


def arrange_kernel(at_ref, near_ref, across_ref, core_ref, *out_refs):
    _, sub, half = near_ref.shape

    def put(row):
        for k, masks in enumerate(SETS):
            for i, m in enumerate(masks):
                for side in range(2):
                    at = (((m >> 1) & 1) * 2 + ((m >> 2) & 1)) * 2 + (m >> 3)
                    if m & 1:
                        block = core_ref[(side ^ row) * 8 + at]
                    else:
                        block = near_ref[at] if side == row else across_ref[at]
                    out_refs[k][i * sub : (i + 1) * sub, side * half : (side + 1) * half] = block

    for row in range(2):
        pl.when(at_ref[1] == row)(functools.partial(put, row))


def bit_order(bit):
    return [4 * z + 2 * x + bit for z in range(4) for x in range(2)]


def local(kernel, outs, *args, spec=None, **extra):
    specs = [SMEM] + [VMEM] * (len(args) - 1) if spec is None else spec
    return pl.pallas_call(
        kernel,
        out_shape=outs,
        in_specs=specs,
        cost_estimate=pl.CostEstimate(flops=1 << 21, bytes_accessed=1 << 20, transcendentals=0),
        compiler_params=pltpu.CompilerParams(vmem_limit_bytes=14 << 20),
        **extra,
    )(*args)


def rows_at(start, count):
    return pl.ds(pl.multiple_of(start, 8), count)


def sum1_kernel(at_ref, own_ref, pre_grad_ref, small_a, small_b, *refs):
    images, (psend, pkeep, qsend, qkeep, total) = refs[:-5], refs[-5:]
    weight_columns(stacked(images), pre_grad_ref, total)
    body, cols = total.shape[0], total.shape[1] // 2
    sub = body // 8
    left, right = pl.ds(0, cols), pl.ds(cols, cols)
    half, row = sub // 2, at_ref[1]
    tail = small_a[...] + small_b[...]
    tail = jnp.concatenate([tail[:4, :cols], tail[:4, cols:]])
    for out, side, across in ((psend, 1 - row, 1), (pkeep, row, 0)):
        for b in range(8):
            rows = rows_at(b * sub + side * half, half)
            out[b * half : (b + 1) * half, :] = own_ref[rows, left] + total[rows, left]
        out[body // 2 :, :] = tail
        out = qsend if out is psend else qkeep
        for z in range(4):
            rows = pl.ds((2 * z + across) * sub, sub)
            out[z * sub : (z + 1) * sub, :] = own_ref[rows, right] + total[rows, right]


def sum2_kernel(at_ref, pa, pb, qa, qb, psend, pkeep, qsend, qkeep):
    body = pa.shape[0] - EXTRA
    half = body // 8
    row = at_ref[1]
    for pout, qout, side, across in ((psend, qsend, 1 - row, 1), (pkeep, qkeep, row, 0)):
        for z in range(4):
            to = pl.ds(z * half, half)
            rows = pl.ds((2 * z + across) * half, half)
            pout[to, :] = pa[rows, :] + pb[rows, :]
            rows = rows_at((2 * z + side) * half, half)
            qout[to, :] = qa[rows, :] + qb[rows, :]
        pout[body // 2 :, :] = pa[body:, :] + pb[body:, :]


def sum3_kernel(at_ref, pa, pb, qa, qb, send, keep):
    body, cols = qa.shape
    half = body // 4
    for out, side in ((send, 1), (keep, 0)):
        for z in range(2):
            to = pl.ds(z * half, half)
            rows = pl.ds((2 * z + side) * half, half)
            out[to, :cols] = pa[rows, :] + pb[rows, :]
            out[to, cols:] = qa[rows, :] + qb[rows, :]
        out[body // 2 :, :cols] = pa[body:, :] + pb[body:, :]
        out[body // 2 :, cols:] = jnp.zeros((EXTRA, cols), F32)


def sum4_kernel(at_ref, a_ref, b_ref, send, keep):
    body = a_ref.shape[0] - EXTRA
    for out, side in ((send, 1), (keep, 0)):
        rows = pl.ds(side * (body // 2), body // 2)
        out[: body // 2, :] = a_ref[rows, :] + b_ref[rows, :]
        out[body // 2 :, :] = a_ref[body:, :] + b_ref[body:, :]


def sum5_kernel(images, at_ref, a_ref, b_ref, part, sums, loss):
    body, cols = part.shape[0], part.shape[1] // 2
    part[...] = (a_ref[:body, :] + b_ref[:body, :]).astype(part.dtype)
    tail = a_ref[body:, :cols] + b_ref[body:, :cols]
    sums[...] = jnp.concatenate([tail[:3], tail[4:7]], axis=1)
    loss[0] = jnp.sum(tail[3:4, :1]) / images


def join_kernel(at_ref, part, other, out):
    half = part.shape[0]
    out[rows_at(at_ref[1] * half, half), :] = part[...].astype(F32)
    out[rows_at((1 - at_ref[1]) * half, half), :] = other[...].astype(F32)


def scatter_steps(at, sources, n, sub, ch):
    f32 = lambda rows, cols: jax.ShapeDtypeStruct((rows, cols), F32)
    cols, half = ch // 2, sub // 2
    on_x = lambda v: exchange(v, "mp", n, 2)
    on_y = lambda v: exchange(v, "dp", 2, 1)
    outs = (f32(8 * half + EXTRA, cols),) * 2 + (f32(4 * sub, cols),) * 2
    psend, pkeep, qsend, qkeep = local(
        sum1_kernel, outs, at, *sources, scratch_shapes=[pltpu.VMEM((8 * sub, ch), F32)]
    )
    parts = pkeep, on_y(psend), qkeep, on_x(qsend)
    outs = (f32(4 * half + EXTRA, cols),) * 2 + (f32(4 * half, cols),) * 2
    psend, pkeep, qsend, qkeep = local(sum2_kernel, outs, at, *parts)
    parts = pkeep, on_x(psend), qkeep, on_y(qsend)
    send, keep = local(sum3_kernel, (f32(2 * half + EXTRA, ch),) * 2, at, *parts)
    arrived = exchange(send, "mp", n, 4)
    send, keep = local(sum4_kernel, (f32(half + EXTRA, ch),) * 2, at, keep, arrived)
    arrived = exchange(send, "mp", n, 8)
    final = jax.ShapeDtypeStruct((half, ch), BF16)
    part, sums, loss = local(
        functools.partial(sum5_kernel, 2 * n),
        (final, f32(3, ch), jax.ShapeDtypeStruct((1,), F32)),
        at,
        keep,
        arrived,
        out_specs=(VMEM, VMEM, SMEM),
    )
    other = on_y(part)
    return local(join_kernel, f32(sub, ch), at, part, other), sums, loss[0]


def land_kernel(masks, at_ref, *refs):
    count = len(masks)
    blocks, out_ref, (wide, sems) = refs[:count], refs[-3], refs[-2:]
    copies = []
    for i, m in enumerate(masks):
        wide[i] = blocks[i][...].astype(F32)
        copies.append(pltpu.make_async_copy(wide.at[i], out_ref.at[at_ref[0] ^ m], sems.at[i]))
        copies[-1].start()
    for copy in copies:
        copy.wait()


def land(at, blocks, masks, out, n):
    sub, cells = blocks[masks[0]].shape
    anywhere = pl.BlockSpec(memory_space=pl.ANY)
    args = [at] + [blocks[m] for m in masks]
    spec = [SMEM] + [VMEM] * len(masks)
    extra = {}
    if out is not None:
        args, spec = args + [out], spec + [anywhere]
        extra["input_output_aliases"] = {len(args) - 1: 0}
    return local(
        functools.partial(land_kernel, masks),
        jax.ShapeDtypeStruct((n, sub, cells), F32),
        *args,
        spec=spec,
        out_specs=anywhere,
        scratch_shapes=[
            pltpu.VMEM((len(masks), sub, cells), F32),
            pltpu.SemaphoreType.DMA((len(masks),)),
        ],
        **extra,
    )


def exchange(value, axis, size, mask):
    return lax.ppermute(value, axis, [(i, i ^ mask) for i in range(size)])


def gather_weight(block, at, n, row):
    sub, ch = block.shape
    half = ch // 2
    rows = lax.dynamic_slice_in_dim(block, row * half, half, 1)[None]
    for mask in (8, 4):
        rows = jnp.concatenate([rows, exchange(rows, "mp", n, mask)])
    near = jnp.concatenate([rows, exchange(rows, "mp", n, 2)])
    across = exchange(near, "dp", 2, 1)
    core = exchange(jnp.concatenate([near, across]), "mp", n, 1)
    outs = tuple(jax.ShapeDtypeStruct((len(m) * sub, ch), BF16) for m in SETS)
    return local(arrange_kernel, outs, at, near, across, core)


def fast_shards(features, conv_weight, norm_gain, norm_bias, logit_vector, labels):
    n, sub, _ = features.shape
    ch = conv_weight.shape[1]
    place, row = lax.axis_index("mp"), lax.axis_index("dp")
    at = jnp.stack([place, row])
    params = jnp.stack([norm_gain, norm_bias, logit_vector])
    params = jnp.broadcast_to(params[:, :, None], (3, ch, 128))
    image = {}
    for m in range(n):
        block = lax.dynamic_index_in_dim(features, place ^ m, 0, keepdims=False)
        image[m] = exchange(block, "mp", n, m) if m else block
    weights = gather_weight(conv_weight, at, n, row)
    pre = None
    for k in PRODUCTS[:2]:
        pre = product(pre, weights[k].T, [image[m] for m in SETS[k]])
        pre, params = lax.optimization_barrier((pre, params))
    twin = [exchange(image[m], "mp", n, 1) for m in bit_order(1)]
    turned = [weights[k].T for k in PRODUCTS[2:]]
    last = [image[m] for k in PRODUCTS[2:] for m in SETS[k]]
    grad_pre, small = head(2 * labels - 1, pre, params, turned, last)
    twin_pre = exchange(grad_pre, "mp", n, 1)
    twin_small = exchange(small, "mp", n, 1)
    blocks = {}
    for k, masks in enumerate(SETS):
        blocks.update(zip(masks, grad_blocks(weights[k], grad_pre, len(masks))))
    landed = {}
    for m, block in blocks.items():
        if m in RELAYED:
            block = exchange(block, "mp", n, m ^ 2)
            landed[m] = exchange(block, "mp", n, 2)
        else:
            landed[m] = exchange(block, "mp", n, m) if m else block
    keep = weight_keep(grad_pre, [image[m] for m in bit_order(0)])
    sources = (keep, twin_pre, small, twin_small, *twin)
    grad_weight, head_grads, loss = scatter_steps(at, sources, n, sub, ch)
    grad_features = None
    for masks in LAND:
        grad_features = land(at, landed, masks, grad_features, n)
    return grad_features, grad_weight, head_grads, loss


def head_total(pre, norm_gain, norm_bias, logit_vector, signs):
    images, channels, cell_count = pre.shape
    grouped = pre.reshape(images, GROUPS, channels // GROUPS, cell_count)
    center = jnp.mean(grouped, axis=(2, 3), keepdims=True)
    spread = jnp.mean((grouped - center) ** 2, axis=(2, 3), keepdims=True)
    normed = ((grouped - center) * lax.rsqrt(spread + norm_eps)).reshape(
        images, channels, cell_count
    )
    normed = normed * norm_gain[:, None] + norm_bias[:, None]
    hidden = jax.nn.silu(normed)
    logits = (
        jnp.einsum("c,ncs->n", logit_vector, hidden, precision=lax.Precision.HIGHEST) / cell_count
    )
    margin = jnp.maximum(1.0 - signs * logits, 0.0)
    return jnp.sum(margin * margin)


def shards(features, conv_weight, norm_gain, norm_bias, logit_vector, labels):
    signs = 2.0 * labels.astype(jnp.float32) - 1.0
    weight_full = lax.all_gather(conv_weight, "mp", axis=0, tiled=True)
    image_block = lax.all_to_all(features, "mp", split_axis=0, concat_axis=1, tiled=True)
    pre = jnp.einsum("io,nis->nos", weight_full, image_block, preferred_element_type=jnp.float32)
    total, pull = jax.vjp(
        lambda p, g, b, h: head_total(p, g, b, h, signs), pre, norm_gain, norm_bias, logit_vector
    )
    grad_pre, grad_gain, grad_bias, grad_vec = pull(jnp.ones((), jnp.float32))
    grad_pre = grad_pre.astype(jnp.bfloat16)
    grad_image = jnp.einsum(
        "io,nos->nis", weight_full, grad_pre, preferred_element_type=jnp.float32
    )
    grad_features = lax.all_to_all(grad_image, "mp", split_axis=1, concat_axis=0, tiled=True)
    weight_term = jnp.einsum(
        "nis,nos->io", image_block, grad_pre, preferred_element_type=jnp.float32
    )
    summed = lax.psum(weight_term, "dp")
    grad_weight = lax.psum_scatter(summed, "mp", scatter_dimension=0, tiled=True)
    total_sum, head_grads = lax.psum(
        (total, jnp.stack([grad_gain, grad_bias, grad_vec])), ("dp", "mp")
    )
    image_total = pre.shape[0] * lax.axis_size("dp") * lax.axis_size("mp")
    loss = total_sum / image_total
    return (grad_features, grad_weight, head_grads, loss)


SETS = ((12, 8, 13, 9), (4, 5, 1, 0), (15, 11, 6, 7), (14, 10, 2, 3))
PRODUCTS = (0, 1, 3, 2)
LAND = ((0, 12, 8, 13, 9), (4, 5, 1, 14, 10), (15, 11, 6, 7, 2, 3))
RELAYED = (14, 10)


def solution(mesh):
    fast = mesh.shape["mp"] == 16 and mesh.shape["dp"] == 2
    return jax.shard_map(
        fast_shards if fast else shards,
        mesh=mesh,
        in_specs=(P("dp", "mp", None), P("mp", None), P(), P(), P(), P(("dp", "mp"))),
        out_specs=(P("dp", "mp", None), P("mp", None), P(), P()),
        check_vma=False,
    )
```

```python
import functools

import jax
import jax.numpy as jnp
from jax import lax
from jax.experimental import pallas as pl
from jax.experimental.pallas import tpu as pltpu
from jax.sharding import PartitionSpec as P

GROUPS = 32
norm_eps = 1e-05
F32 = jnp.float32
BF16 = jnp.bfloat16
VMEM = pl.BlockSpec(memory_space=pltpu.VMEM)
SMEM = pl.BlockSpec(memory_space=pltpu.SMEM)
EXTRA = 8


def stacked(refs):
    return jnp.concatenate([ref[...] for ref in refs])


def weight_columns(rows, grad_pre, out):
    ch = grad_pre.shape[0]
    step = ch // 5
    for j in range(5):
        cols = pl.ds(j * step, step)
        out[: rows.shape[0], cols] = lax.dot_general(
            rows, grad_pre[cols, :], (((1,), (1,)), ((), ())), preferred_element_type=F32
        )


def head_kernel(
    info_ref, begun_ref, par_ref, weight_ref, weight_too_ref, *refs,
):
    last_refs, last_too_refs, refs = refs[:4], refs[4:8], refs[8:]
    pre_grad_ref, small_ref, pre_ref, slope_ref, sums_ref, center_ref, rstd_ref = refs
    ch, cells = pre_ref.shape
    width = ch // GROUPS
    count = width * cells
    add_product(begun_ref, weight_ref, last_refs, pre_ref)
    add_product(pre_ref, weight_too_ref, last_too_refs, pre_ref)

    def at(g):
        return pl.ds(pl.multiple_of(g * width, 8), width)

    def tile(g, r):
        return pl.ds(pl.multiple_of(g * width + 8 * r, 8), 8)

    tiles, lanes = range(width // 8), [pl.ds(128 * c, 128) for c in range(cells // 128)]

    def sweep(body, trips, unroll):
        lax.fori_loop(0, trips, lambda g, _: body(g) or 0, 0, unroll=unroll)

    def spot(value):
        return jnp.broadcast_to(value, (8, 128))

    def means(g):
        center_ref[g] = spot(jnp.sum(pre_ref[at(g), :], axis=(0, 1), keepdims=True) / count)

    def spreads(g):
        center, acc = center_ref[g], jnp.zeros((8, 128), F32)
        for r in tiles:
            for c in lanes:
                dev = pre_ref[tile(g, r), c] - center
                acc += dev * dev
        spread = jnp.sum(acc, axis=(0, 1), keepdims=True) / count
        rstd_ref[g] = spot(lax.rsqrt(spread + norm_eps))

    def activate(g):
        center, rstd = center_ref[g], rstd_ref[g]
        for r in tiles:
            rows = tile(g, r)
            a, b = par_ref[0, rows, :] * (0.5 * rstd), 0.5 * par_ref[1, rows, :]
            sum_h = sum_d = sum_du = jnp.zeros((8, 128), F32)
            for c in lanes:
                dev = pre_ref[rows, c] - center
                w = dev * a + b
                t = jnp.tanh(w)
                q = 1.0 + t
                h = w * q
                d2 = q + h * (1.0 - t)
                slope_ref[rows, c] = d2
                sum_h += h
                sum_d += d2
                sum_du += d2 * dev
            sums_ref[0, rows, :] = sum_du * (0.5 * rstd)
            sums_ref[1, rows, :] = 0.5 * sum_d
            sums_ref[2, rows, :] = sum_h

    sweep(means, GROUPS, 8)
    sweep(spreads, GROUPS, 8)
    sweep(activate, GROUPS, 2)

    def total(g):
        for i in range(3):
            lane_sum = jnp.sum(sums_ref[i, at(g), :], axis=1, keepdims=True)
            sums_ref[i, at(g), :] = jnp.broadcast_to(lane_sum, (width, 128))

    sweep(total, GROUPS, 8)
    logit = jnp.sum(par_ref[2] * sums_ref[2], axis=0, keepdims=True) / cells
    sign = info_ref[0].astype(F32)
    margin = jnp.maximum(1.0 - sign * logit, 0.0)
    k = (-2.0 * sign / cells) * margin

    def finish(pair):
        out = {}
        for side in range(2):
            g = 2 * pair + side
            center, rstd = center_ref[g], rstd_ref[g]
            gv = par_ref[0, at(g), :] * par_ref[2, at(g), :]
            scale = (k / count) * rstd
            m1 = scale * jnp.sum(gv * sums_ref[1, at(g), :], axis=0, keepdims=True)
            m2 = scale * rstd * jnp.sum(gv * sums_ref[0, at(g), :], axis=0, keepdims=True)
            for r in tiles:
                rows = tile(g, r)
                slope = (0.5 * k) * rstd * (par_ref[0, rows, :] * par_ref[2, rows, :])
                for i, c in enumerate(lanes):
                    dev = pre_ref[rows, c] - center
                    out[side * len(tiles) + r, i] = slope_ref[rows, c] * slope - (m1 + dev * m2)
        for r in tiles:
            rows = pl.ds(pl.multiple_of(2 * pair * width + 16 * r, 16), 16)
            for i, c in enumerate(lanes):
                both = jnp.concatenate([out[2 * r, i], out[2 * r + 1, i]])
                pre_grad_ref[rows, c] = both.astype(BF16)

    sweep(finish, GROUPS // 2, 1)
    lane = lax.broadcasted_iota(jnp.int32, (ch, 128), 1)
    vec = par_ref[2]
    turned = jnp.where(lane == 0, vec * sums_ref[0], 0.0)
    turned = jnp.where(lane == 1, vec * sums_ref[1], turned)
    turned = jnp.where(lane == 2, sums_ref[2], turned).T[:EXTRA]
    line = lax.broadcasted_iota(jnp.int32, turned.shape, 0)
    k, margin = k[:, :1], margin[:, :1]
    small_ref[...] = jnp.where(line == 3, margin * margin, turned * k)


def head(sign, begun, params, turned, last):
    ch, cells = begun.shape
    return pl.pallas_call(
        head_kernel,
        out_shape=(jax.ShapeDtypeStruct((ch, cells), BF16), jax.ShapeDtypeStruct((EXTRA, ch), F32)),
        in_specs=[SMEM] + [VMEM] * 12,
        out_specs=(VMEM, VMEM),
        scratch_shapes=[pltpu.VMEM((ch, cells), F32)] * 2
        + [pltpu.VMEM((3, ch, 128), F32)]
        + [pltpu.VMEM((GROUPS, 8, 128), F32)] * 2,
        cost_estimate=pl.CostEstimate(
            flops=3 * ch * ch * cells, bytes_accessed=8 * ch * cells, transcendentals=ch * cells
        ),
        compiler_params=pltpu.CompilerParams(vmem_limit_bytes=28 << 20),
        name="head",
    )(sign, begun, params, *turned, *last)


def add_product(begun_ref, weight_ref, refs, out_ref):
    image = stacked(refs)
    step = out_ref.shape[0] // 2
    for j in range(2):
        rows = pl.ds(j * step, step)
        product = lax.dot_general(
            weight_ref[:, rows], image, (((0,), (0,)), ((), ())), preferred_element_type=F32
        )
        out_ref[rows, :] = product if begun_ref is None else begun_ref[rows, :] + product


def first_kernel(weight_ref, *refs):
    add_product(None, weight_ref, refs[:-1], refs[-1])


def next_kernel(begun_ref, weight_ref, *refs):
    add_product(begun_ref, weight_ref, refs[:-1], refs[-1])


def product(begun, turned, images):
    depth, ch = turned.shape
    cells = images[0].shape[1]
    args = ([] if begun is None else [begun]) + [turned, *images]
    return pl.pallas_call(
        first_kernel if begun is None else next_kernel,
        out_shape=jax.ShapeDtypeStruct((ch, cells), F32),
        in_specs=[VMEM] * len(args),
        out_specs=VMEM,
        input_output_aliases={} if begun is None else {0: 0},
        cost_estimate=pl.CostEstimate(
            flops=2 * ch * depth * cells, bytes_accessed=8 * ch * cells, transcendentals=0
        ),
        compiler_params=pltpu.CompilerParams(vmem_limit_bytes=14 << 20),
        name="product",
    )(*args)


def image_kernel(weight_ref, pre_grad_ref, *out_refs):
    sub = out_refs[0].shape[0]
    grads = jnp.dot(weight_ref[...], pre_grad_ref[...], preferred_element_type=F32)
    for i, out_ref in enumerate(out_refs):
        out_ref[...] = grads[i * sub : (i + 1) * sub].astype(BF16)


def grad_blocks(weight, grad_pre, parts):
    rows, ch = weight.shape
    cells = grad_pre.shape[1]
    return pl.pallas_call(
        image_kernel,
        out_shape=(jax.ShapeDtypeStruct((rows // parts, cells), BF16),) * parts,
        in_specs=[VMEM, VMEM],
        out_specs=(VMEM,) * parts,
        cost_estimate=pl.CostEstimate(
            flops=2 * rows * ch * cells, bytes_accessed=2 * ch * cells, transcendentals=0
        ),
        compiler_params=pltpu.CompilerParams(vmem_limit_bytes=12 << 20),
        name="grad_blocks",
    )(weight, grad_pre)


def keep_kernel(pre_grad_ref, *refs):
    weight_columns(stacked(refs[:-1]), pre_grad_ref, refs[-1])


def weight_keep(grad_pre, images):
    ch, cells = grad_pre.shape
    return pl.pallas_call(
        keep_kernel,
        out_shape=jax.ShapeDtypeStruct((ch // 2, ch), F32),
        in_specs=[VMEM] * (1 + len(images)),
        out_specs=VMEM,
        cost_estimate=pl.CostEstimate(
            flops=ch * ch * cells, bytes_accessed=4 * ch * cells, transcendentals=0
        ),
        compiler_params=pltpu.CompilerParams(vmem_limit_bytes=14 << 20),
        name="weight_keep",
    )(grad_pre, *images)


def arrange_kernel(at_ref, near_ref, across_ref, core_ref, *out_refs):
    _, sub, half = near_ref.shape

    def put(row):
        for k, masks in enumerate(SETS):
            for i, m in enumerate(masks):
                for side in range(2):
                    at = (((m >> 1) & 1) * 2 + ((m >> 2) & 1)) * 2 + (m >> 3)
                    if m & 1:
                        block = core_ref[(side ^ row) * 8 + at]
                    else:
                        block = near_ref[at] if side == row else across_ref[at]
                    out_refs[k][i * sub : (i + 1) * sub, side * half : (side + 1) * half] = block

    for row in range(2):
        pl.when(at_ref[1] == row)(functools.partial(put, row))


def bit_order(bit):
    return [4 * z + 2 * x + bit for z in range(4) for x in range(2)]


def local(kernel, outs, *args, spec=None, **extra):
    specs = [SMEM] + [VMEM] * (len(args) - 1) if spec is None else spec
    return pl.pallas_call(
        kernel,
        out_shape=outs,
        in_specs=specs,
        cost_estimate=pl.CostEstimate(flops=1 << 21, bytes_accessed=1 << 20, transcendentals=0),
        compiler_params=pltpu.CompilerParams(vmem_limit_bytes=14 << 20),
        **extra,
    )(*args)


def rows_at(start, count):
    return pl.ds(pl.multiple_of(start, 8), count)


def sum1_kernel(at_ref, own_ref, pre_grad_ref, small_a, small_b, *refs):
    images, (psend, pkeep, qsend, qkeep, total) = refs[:-5], refs[-5:]
    weight_columns(stacked(images), pre_grad_ref, total)
    body, cols = total.shape[0], total.shape[1] // 2
    sub = body // 8
    left, right = pl.ds(0, cols), pl.ds(cols, cols)
    half, row = sub // 2, at_ref[1]
    tail = small_a[...] + small_b[...]
    tail = jnp.concatenate([tail[:4, :cols], tail[:4, cols:]])
    for out, side, across in ((psend, 1 - row, 1), (pkeep, row, 0)):
        for b in range(8):
            rows = rows_at(b * sub + side * half, half)
            out[b * half : (b + 1) * half, :] = own_ref[rows, left] + total[rows, left]
        out[body // 2 :, :] = tail
        out = qsend if out is psend else qkeep
        for z in range(4):
            rows = pl.ds((2 * z + across) * sub, sub)
            out[z * sub : (z + 1) * sub, :] = own_ref[rows, right] + total[rows, right]


def sum2_kernel(at_ref, pa, pb, qa, qb, psend, pkeep, qsend, qkeep):
    body = pa.shape[0] - EXTRA
    half = body // 8
    row = at_ref[1]
    for pout, qout, side, across in ((psend, qsend, 1 - row, 1), (pkeep, qkeep, row, 0)):
        for z in range(4):
            to = pl.ds(z * half, half)
            rows = pl.ds((2 * z + across) * half, half)
            pout[to, :] = pa[rows, :] + pb[rows, :]
            rows = rows_at((2 * z + side) * half, half)
            qout[to, :] = qa[rows, :] + qb[rows, :]
        pout[body // 2 :, :] = pa[body:, :] + pb[body:, :]


def sum3_kernel(at_ref, pa, pb, qa, qb, send, keep):
    body, cols = qa.shape
    half = body // 4
    for out, side in ((send, 1), (keep, 0)):
        for z in range(2):
            to = pl.ds(z * half, half)
            rows = pl.ds((2 * z + side) * half, half)
            out[to, :cols] = pa[rows, :] + pb[rows, :]
            out[to, cols:] = qa[rows, :] + qb[rows, :]
        out[body // 2 :, :cols] = pa[body:, :] + pb[body:, :]
        out[body // 2 :, cols:] = jnp.zeros((EXTRA, cols), F32)


def sum4_kernel(at_ref, a_ref, b_ref, send, keep):
    body = a_ref.shape[0] - EXTRA
    for out, side in ((send, 1), (keep, 0)):
        rows = pl.ds(side * (body // 2), body // 2)
        out[: body // 2, :] = a_ref[rows, :] + b_ref[rows, :]
        out[body // 2 :, :] = a_ref[body:, :] + b_ref[body:, :]


def sum5_kernel(images, at_ref, a_ref, b_ref, part, sums, loss):
    body, cols = part.shape[0], part.shape[1] // 2
    part[...] = (a_ref[:body, :] + b_ref[:body, :]).astype(part.dtype)
    tail = a_ref[body:, :cols] + b_ref[body:, :cols]
    sums[...] = jnp.concatenate([tail[:3], tail[4:7]], axis=1)
    loss[0] = jnp.sum(tail[3:4, :1]) / images


def join_kernel(at_ref, part, other, out):
    half = part.shape[0]
    out[rows_at(at_ref[1] * half, half), :] = part[...].astype(F32)
    out[rows_at((1 - at_ref[1]) * half, half), :] = other[...].astype(F32)


def scatter_steps(at, sources, n, sub, ch):
    f32 = lambda rows, cols: jax.ShapeDtypeStruct((rows, cols), F32)
    cols, half = ch // 2, sub // 2
    on_x = lambda v: exchange(v, "mp", n, 2)
    on_y = lambda v: exchange(v, "dp", 2, 1)
    outs = (f32(8 * half + EXTRA, cols),) * 2 + (f32(4 * sub, cols),) * 2
    psend, pkeep, qsend, qkeep = local(
        sum1_kernel, outs, at, *sources, scratch_shapes=[pltpu.VMEM((8 * sub, ch), F32)]
    )
    parts = pkeep, on_y(psend), qkeep, on_x(qsend)
    outs = (f32(4 * half + EXTRA, cols),) * 2 + (f32(4 * half, cols),) * 2
    psend, pkeep, qsend, qkeep = local(sum2_kernel, outs, at, *parts)
    parts = pkeep, on_x(psend), qkeep, on_y(qsend)
    send, keep = local(sum3_kernel, (f32(2 * half + EXTRA, ch),) * 2, at, *parts)
    arrived = exchange(send, "mp", n, 4)
    send, keep = local(sum4_kernel, (f32(half + EXTRA, ch),) * 2, at, keep, arrived)
    arrived = exchange(send, "mp", n, 8)
    final = jax.ShapeDtypeStruct((half, ch), BF16)
    part, sums, loss = local(
        functools.partial(sum5_kernel, 2 * n),
        (final, f32(3, ch), jax.ShapeDtypeStruct((1,), F32)),
        at,
        keep,
        arrived,
        out_specs=(VMEM, VMEM, SMEM),
    )
    other = on_y(part)
    return local(join_kernel, f32(sub, ch), at, part, other), sums, loss[0]


def land_kernel(masks, at_ref, *refs):
    count = len(masks)
    blocks, out_ref, (wide, sems) = refs[:count], refs[-3], refs[-2:]
    copies = []
    for i, m in enumerate(masks):
        wide[i] = blocks[i][...].astype(F32)
        copies.append(pltpu.make_async_copy(wide.at[i], out_ref.at[at_ref[0] ^ m], sems.at[i]))
        copies[-1].start()
    for copy in copies:
        copy.wait()


def land(at, blocks, masks, out, n):
    sub, cells = blocks[masks[0]].shape
    anywhere = pl.BlockSpec(memory_space=pl.ANY)
    args = [at] + [blocks[m] for m in masks]
    spec = [SMEM] + [VMEM] * len(masks)
    extra = {}
    if out is not None:
        args, spec = args + [out], spec + [anywhere]
        extra["input_output_aliases"] = {len(args) - 1: 0}
    return local(
        functools.partial(land_kernel, masks),
        jax.ShapeDtypeStruct((n, sub, cells), F32),
        *args,
        spec=spec,
        out_specs=anywhere,
        scratch_shapes=[
            pltpu.VMEM((len(masks), sub, cells), F32),
            pltpu.SemaphoreType.DMA((len(masks),)),
        ],
        **extra,
    )


def exchange(value, axis, size, mask):
    return lax.ppermute(value, axis, [(i, i ^ mask) for i in range(size)])


def gather_weight(block, at, n, row):
    sub, ch = block.shape
    half = ch // 2
    rows = lax.dynamic_slice_in_dim(block, row * half, half, 1)[None]
    for mask in (8, 4):
        rows = jnp.concatenate([rows, exchange(rows, "mp", n, mask)])
    near = jnp.concatenate([rows, exchange(rows, "mp", n, 2)])
    across = exchange(near, "dp", 2, 1)
    core = exchange(jnp.concatenate([near, across]), "mp", n, 1)
    outs = tuple(jax.ShapeDtypeStruct((len(m) * sub, ch), BF16) for m in SETS)
    return local(arrange_kernel, outs, at, near, across, core)


def fast_shards(features, conv_weight, norm_gain, norm_bias, logit_vector, labels):
    n, sub, _ = features.shape
    ch = conv_weight.shape[1]
    place, row = lax.axis_index("mp"), lax.axis_index("dp")
    at = jnp.stack([place, row])
    params = jnp.stack([norm_gain, norm_bias, logit_vector])
    params = jnp.broadcast_to(params[:, :, None], (3, ch, 128))
    image = {}
    for m in range(n):
        block = lax.dynamic_index_in_dim(features, place ^ m, 0, keepdims=False)
        image[m] = exchange(block, "mp", n, m) if m else block
    weights = gather_weight(conv_weight, at, n, row)
    pre = None
    for k in PRODUCTS[:2]:
        pre = product(pre, weights[k], [image[m] for m in SETS[k]])
        pre, params = lax.optimization_barrier((pre, params))
    twin = [exchange(image[m], "mp", n, 1) for m in bit_order(1)]
    turned = [weights[k] for k in PRODUCTS[2:]]
    last = [image[m] for k in PRODUCTS[2:] for m in SETS[k]]
    grad_pre, small = head(2 * labels - 1, pre, params, turned, last)
    twin_pre = exchange(grad_pre, "mp", n, 1)
    twin_small = exchange(small, "mp", n, 1)
    blocks = {}
    for k, masks in enumerate(SETS):
        blocks.update(zip(masks, grad_blocks(weights[k], grad_pre, len(masks))))
    landed = {}
    for m, block in blocks.items():
        if m in RELAYED:
            block = exchange(block, "mp", n, m ^ 2)
            landed[m] = exchange(block, "mp", n, 2)
        else:
            landed[m] = exchange(block, "mp", n, m) if m else block
    keep = weight_keep(grad_pre, [image[m] for m in bit_order(0)])
    sources = (keep, twin_pre, small, twin_small, *twin)
    grad_weight, head_grads, loss = scatter_steps(at, sources, n, sub, ch)
    grad_features = None
    for masks in LAND:
        grad_features = land(at, landed, masks, grad_features, n)
    return grad_features, grad_weight, head_grads, loss


def head_total(pre, norm_gain, norm_bias, logit_vector, signs):
    images, channels, cell_count = pre.shape
    grouped = pre.reshape(images, GROUPS, channels // GROUPS, cell_count)
    center = jnp.mean(grouped, axis=(2, 3), keepdims=True)
    spread = jnp.mean((grouped - center) ** 2, axis=(2, 3), keepdims=True)
    normed = ((grouped - center) * lax.rsqrt(spread + norm_eps)).reshape(
        images, channels, cell_count
    )
    normed = normed * norm_gain[:, None] + norm_bias[:, None]
    hidden = jax.nn.silu(normed)
    logits = (
        jnp.einsum("c,ncs->n", logit_vector, hidden, precision=lax.Precision.HIGHEST) / cell_count
    )
    margin = jnp.maximum(1.0 - signs * logits, 0.0)
    return jnp.sum(margin * margin)


def shards(features, conv_weight, norm_gain, norm_bias, logit_vector, labels):
    signs = 2.0 * labels.astype(jnp.float32) - 1.0
    weight_full = lax.all_gather(conv_weight, "mp", axis=0, tiled=True)
    image_block = lax.all_to_all(features, "mp", split_axis=0, concat_axis=1, tiled=True)
    pre = jnp.einsum("io,nis->nos", weight_full, image_block, preferred_element_type=jnp.float32)
    total, pull = jax.vjp(
        lambda p, g, b, h: head_total(p, g, b, h, signs), pre, norm_gain, norm_bias, logit_vector
    )
    grad_pre, grad_gain, grad_bias, grad_vec = pull(jnp.ones((), jnp.float32))
    grad_pre = grad_pre.astype(jnp.bfloat16)
    grad_image = jnp.einsum(
        "io,nos->nis", weight_full, grad_pre, preferred_element_type=jnp.float32
    )
    grad_features = lax.all_to_all(grad_image, "mp", split_axis=1, concat_axis=0, tiled=True)
    weight_term = jnp.einsum(
        "nis,nos->io", image_block, grad_pre, preferred_element_type=jnp.float32
    )
    summed = lax.psum(weight_term, "dp")
    grad_weight = lax.psum_scatter(summed, "mp", scatter_dimension=0, tiled=True)
    total_sum, head_grads = lax.psum(
        (total, jnp.stack([grad_gain, grad_bias, grad_vec])), ("dp", "mp")
    )
    image_total = pre.shape[0] * lax.axis_size("dp") * lax.axis_size("mp")
    loss = total_sum / image_total
    return (grad_features, grad_weight, head_grads, loss)


SETS = ((12, 8, 13, 9), (4, 5, 1, 0), (15, 11, 6, 7), (14, 10, 2, 3))
PRODUCTS = (0, 1, 3, 2)
LAND = ((0, 12, 8, 13, 9), (4, 5, 1, 14, 10), (15, 11, 6, 7, 2, 3))
RELAYED = (14, 10)


def solution(mesh):
    fast = mesh.shape["mp"] == 16 and mesh.shape["dp"] == 2
    return jax.shard_map(
        fast_shards if fast else shards,
        mesh=mesh,
        in_specs=(P("dp", "mp", None), P("mp", None), P(), P(), P(), P(("dp", "mp"))),
        out_specs=(P("dp", "mp", None), P("mp", None), P(), P()),
        check_vma=False,
    )
```
